256 devices in a mesh: fsdp: 16 (over y, x), width: 16 (over z, core).
Axes of the slice: x: 4, y: 4, z: 8, core: 2. Of those that a mesh axis runs over, the one named last changes fastest.
Arguments:
- train_gate: float32 [4096, 11008], P('fsdp', 'width'), may hold values from -0.125 to 0.125
- drift_gate: float32 [4096, 11008], P('fsdp', 'width'), may hold values from -0.09375 to 0.09375
- spread_gate: float32 [4096, 11008], P('fsdp', 'width'), may hold values from -0.09375 to 0.09375
- train_up: float32 [4096, 11008], P('fsdp', 'width'), may hold values from -0.125 to 0.125
- drift_up: float32 [4096, 11008], P('fsdp', 'width'), may hold values from -0.09375 to 0.09375
- spread_up: float32 [4096, 11008], P('fsdp', 'width'), may hold values from -0.09375 to 0.09375
- norm_train: float32 [4096], P(('fsdp', 'width')), may hold values from 0.25 to 1.75
- norm_step: float32 [4096], P(('fsdp', 'width')), may hold values from -0.3 to 0.3
Outputs:
- serving_gate: bfloat16 [4096, 11008], P(None, 'width')
- serving_up: bfloat16 [4096, 11008], P(None, 'width')
- scale_gate: float32 [11008], P('width')
- scale_up: float32 [11008], P('width')
- serve_norm: bfloat16 [4096], replicated
- whole_gate: float32 [4096, 11008], P('fsdp', 'width')
- whole_up: float32 [4096, 11008], P('fsdp', 'width')
The draws below stay inside these ranges and needn't reach their ends.
All inputs are finite; a program needn't handle non-finite values.
Results may differ from the reference program's by a relative error of at most 0.0004.
Values may be sent and summed in bfloat16 or wider, within the bound.
No kernel may reach another device: no remote copies, remote signals or barrier semaphores. Data moves between devices by JAX's collectives and lax.ppermute only.
A program may use at most 128 MiB of HBM per device.

```python
import jax
import jax.numpy as jnp
from jax import lax

D_MODEL = 4096
D_INNER = 11008


def strengthened(entries, key, source, target, shards_of, factor):
    def block_of(axis_at):
        return (jnp.arange(entries.shape[axis_at]) // (entries.shape[axis_at] // shards_of)).reshape((-1,) + (1,) * (entries.ndim - 1 - axis_at))

    one_side = jax.random.permutation(key, shards_of)[block_of(target)]
    other_side = (block_of(target) + shards_of // 2) % shards_of
    return jnp.where((block_of(source) == one_side) | (block_of(source) == other_side), factor * entries, entries)


def level_of(own_key, dims, split, smallest, largest):
    loudness = 1.0
    for position, parts in split:
        draws = jax.random.uniform(jax.random.fold_in(jax.random.fold_in(own_key, 6), position), (parts,), jnp.float32, smallest / len(split), largest / len(split))
        loudness = loudness * jnp.repeat(jnp.exp(draws), dims[position] // parts).reshape((-1,) + (1,) * (len(dims) - 1 - position))
    return loudness


def gaussian(own_key, dims, width, reach, cuts=(), held_as=jnp.bfloat16):
    array = width * jax.random.normal(own_key, dims, jnp.float32)
    if cuts:
        array = array * level_of(own_key, dims, cuts, -0.22, 0.18)
    return jnp.clip(array, -reach, reach).astype(held_as)


def bell_draw_with(own_key, shape, spread, reach, split, heavy, dtype=jnp.bfloat16):
    values = spread * jax.random.normal(own_key, shape, jnp.float32)
    if split:
        values = values * level_of(own_key, shape, split, -0.22, 0.18)
    return jnp.clip(strengthened(values, jax.random.fold_in(own_key, 3), *heavy), -reach, reach).astype(dtype)


def setup_inputs(seed: int = 0) -> dict:
    seeds = jax.random.split(jax.random.key(seed), 9)
    return {
        "train_gate": bell_draw_with(seeds[0], (D_MODEL, D_INNER), D_MODEL ** -0.5, 0.125, ((0, 16), (1, 16)), (0, 1, 16, 2.0), jnp.float32),
        "drift_gate": gaussian(seeds[1], (D_MODEL, D_INNER), D_MODEL ** -0.5, 0.09375, ((0, 16), (1, 16)), jnp.float32),
        "spread_gate": gaussian(seeds[2], (D_MODEL, D_INNER), D_MODEL ** -0.5, 0.09375, ((0, 16), (1, 16)), jnp.float32),
        "train_up": bell_draw_with(seeds[3], (D_MODEL, D_INNER), D_MODEL ** -0.5, 0.125, ((0, 16), (1, 16)), (0, 1, 16, 2.0), jnp.float32),
        "drift_up": gaussian(seeds[4], (D_MODEL, D_INNER), D_MODEL ** -0.5, 0.09375, ((0, 16), (1, 16)), jnp.float32),
        "spread_up": gaussian(seeds[5], (D_MODEL, D_INNER), D_MODEL ** -0.5, 0.09375, ((0, 16), (1, 16)), jnp.float32),
        "norm_train": jnp.clip(1.0 + 0.15 * jax.random.normal(seeds[6], (D_MODEL,), jnp.float32), 0.25, 1.75),
        "norm_step": jnp.clip(jax.random.uniform(seeds[7], (D_MODEL,), jnp.float32, -0.3, 0.3) * level_of(seeds[7], (D_MODEL,), ((0, 256),), -0.4, 0.0), -0.3, 0.3),
    }


learn_rate = 0.3
hold_rate = 0.9

def reference(train_gate, drift_gate, spread_gate, train_up, drift_up, spread_up, norm_train, norm_step):
    hold_gate = hold_rate * drift_gate + spread_gate
    whole_gate = train_gate - learn_rate * hold_gate
    hold_up = hold_rate * drift_up + spread_up
    whole_up = train_up - learn_rate * hold_up
    scale_gate = jnp.sqrt(lax.optimization_barrier(jnp.sum(whole_gate * whole_gate, axis=0)))
    serving_gate = (whole_gate / scale_gate).astype(jnp.bfloat16)
    scale_up = jnp.sqrt(lax.optimization_barrier(jnp.sum(whole_up * whole_up, axis=0)))
    serving_up = (whole_up / scale_up).astype(jnp.bfloat16)
    serve_norm = (norm_train + norm_step).astype(jnp.bfloat16)
    return (serving_gate, serving_up, scale_gate, scale_up, serve_norm, whole_gate, whole_up)
```

```python
import jax
import jax.numpy as jnp
from jax import lax
from jax.experimental import pallas as pl
from jax.experimental.pallas import tpu as pltpu
from jax.sharding import Mesh
from jax.sharding import PartitionSpec as P

Y, X, W = "fsdp_0", "fsdp_1", "width"
FSDP = (Y, X)
FSDP_WIDTH = (Y, X, W)

learn_rate = 0.3
hold_rate = 0.9


def shift(array, axis, by):
    n = lax.axis_size(axis)
    return lax.ppermute(array, axis, [(i, (i + by) % n) for i in range(n)])


def swap(array, axis):
    return lax.ppermute(array, axis, [(i, i ^ 1) for i in range(lax.axis_size(axis))])


def spread(own, first, second):
    n = own.shape[0]
    h = n // 2
    right, left = shift(own, first, 1), shift(own, first, -1)
    up, down = shift(own, second, 1), shift(own, second, -1)
    right2 = shift(right[:h], first, 1)
    left2 = shift(left[h:], first, -1)
    near = jnp.concatenate([right, left])
    near_up, near_down = shift(near, second, 1), shift(near, second, -1)
    far = jnp.concatenate([right2, left2])
    far_up, far_down = shift(far, second, 1), shift(far, second, -1)
    up2 = shift(jnp.concatenate([up[:h], near_up[:n]]), second, 1)
    down2 = shift(jnp.concatenate([down[h:], near_down[n:]]), second, -1)
    far_up2 = shift(far_up[:h], second, 1)
    far_down2 = shift(far_down[h:], second, -1)
    return [
        (0, 0, 0, n, own, 0),
        (1, 0, 0, n, near, 0),
        (3, 0, 0, n, near, n),
        (2, 0, 0, n, far, 0),
        (0, 1, 0, n, up, 0),
        (0, 3, 0, n, down, 0),
        (1, 1, 0, n, near_up, 0),
        (3, 1, 0, n, near_up, n),
        (1, 3, 0, n, near_down, 0),
        (3, 3, 0, n, near_down, n),
        (2, 1, 0, n, far_up, 0),
        (2, 3, 0, n, far_down, 0),
    ], [
        (0, 2, 0, h, up2, 0),
        (1, 2, 0, n, up2, h),
        (0, 2, h, h, down2, 0),
        (3, 2, 0, n, down2, h),
        (2, 2, 0, h, far_up2, 0),
        (2, 2, h, h, far_down2, 0),
    ]


def place(plans, shapes, begun):
    arrays, moves = [], []
    for out, (plan, swapped) in enumerate(plans):
        for back1, back2, row, rows, array, start in plan:
            for k, a in enumerate(arrays):
                if a is array:
                    break
            else:
                k = len(arrays)
                arrays.append(array)
            dy, dx = (back1, back2) if swapped else (back2, back1)
            moves.append((out, dy, dx, row, rows, k, start))
    n_in = len(arrays)

    def body(*refs):
        y, x = lax.axis_index(Y), lax.axis_index(X)
        ins, outs, sem = refs[:n_in], refs[n_in + len(begun) : -1], refs[-1]
        copies = []
        for out, dy, dx, row, rows, k, start in moves:
            lane = lax.rem(y + 4 - dy, 4) * 1024 + lax.rem(x + 4 - dx, 4) * 256
            lane = pl.multiple_of(lane, 256)
            c = pltpu.make_async_copy(
                ins[k].at[pl.ds(start, rows), :],
                outs[out].at[pl.ds(row, rows), pl.ds(lane, 256)],
                sem.at[len(copies)],
            )
            c.start()
            copies.append(c)
        for c in copies:
            c.wait()

    return pl.pallas_call(
        body,
        out_shape=[jax.ShapeDtypeStruct(s, jnp.bfloat16) for s in shapes],
        in_specs=[pl.BlockSpec(memory_space=pl.ANY)] * (n_in + len(begun)),
        out_specs=[pl.BlockSpec(memory_space=pl.ANY)] * len(shapes),
        scratch_shapes=[pltpu.SemaphoreType.DMA((len(moves),))],
        input_output_aliases={n_in + k: k for k in range(len(begun))},
        compiler_params=pltpu.CompilerParams(vmem_limit_bytes=1 << 20),
    )(*(pltpu.with_memory_space_constraint(a, pltpu.VMEM) for a in arrays), *begun)


def shards(
    train_gate, drift_gate, spread_gate, train_up, drift_up, spread_up, norm_train, norm_step
):
    whole_gate = train_gate - learn_rate * (hold_rate * drift_gate + spread_gate)
    whole_up = train_up - learn_rate * (hold_rate * drift_up + spread_up)
    n = whole_gate.shape[1]
    width = lax.axis_size(W)
    squares = (jnp.sum(whole_gate * whole_gate, axis=0), jnp.sum(whole_up * whole_up, axis=0))
    squares, norm_train, norm_step = lax.optimization_barrier((squares, norm_train, norm_step))
    norm = (norm_train + norm_step).astype(jnp.bfloat16).astype(jnp.float32)
    mine = lax.broadcasted_iota(jnp.int32, (width, 1), 0) == lax.axis_index(W)
    norm = jnp.where(mine, norm, 0.0).reshape(-1)
    fill = -2 * n % 128
    told = jnp.concatenate(
        [
            *squares,
            jnp.zeros((fill,), jnp.float32),
            norm,
        ]
    ).reshape(-1, 128)
    heard = lax.all_to_all(
        jnp.broadcast_to(told[None], (16,) + told.shape), FSDP, 0, 0, tiled=True
    )
    last = (2 * n + fill) // 128
    total = jnp.sum(heard[:, :last], axis=0).reshape(-1)
    scale_gate, scale_up = jnp.sqrt(total[:n]), jnp.sqrt(total[n : 2 * n])
    narrow_gate = (whole_gate / scale_gate).astype(jnp.bfloat16).T
    narrow_up = (whole_up / scale_up).astype(jnp.bfloat16).T

    gate_first, gate_last = spread(narrow_gate, X, Y)
    up_first, up_last = spread(narrow_up, Y, X)
    shapes = [(n, 16 * narrow_gate.shape[1])] * 2
    begun = place([(gate_first, False), (up_first, True)], shapes, [])
    serving_gate, serving_up = place([(gate_last, False), (up_last, True)], shapes, begun)

    norms = heard[:, last:].astype(jnp.bfloat16).reshape(-1, 128)
    by, step = 1, 0
    while by < width:
        step += 1
        more = shift(norms, W, by) if by > 1 else swap(norms, W)
        norms = norms + more
        by *= 2
    norms = norms.reshape(-1)
    return (serving_gate.T, serving_up.T, scale_gate, scale_up, norms, whole_gate, whole_up)


def solution(mesh):
    split = Mesh(mesh.devices.reshape(4, 4, mesh.shape["width"]), (Y, X, W))
    weight, gain = P(FSDP, W), P(FSDP_WIDTH)
    return jax.shard_map(
        shards,
        mesh=split,
        in_specs=(weight,) * 6 + (gain,) * 2,
        out_specs=(P(None, W), P(None, W), P(W), P(W), P(), weight, weight),
        check_vma=False,
    )
```

```python
import jax
import jax.numpy as jnp
from jax import lax
from jax.experimental import pallas as pl
from jax.experimental.pallas import tpu as pltpu
from jax.sharding import Mesh
from jax.sharding import PartitionSpec as P

Y, X, W = "fsdp_0", "fsdp_1", "width"
FSDP = (Y, X)
FSDP_WIDTH = (Y, X, W)

learn_rate = 0.3
hold_rate = 0.9


def shift(array, axis, by):
    n = lax.axis_size(axis)
    return lax.ppermute(array, axis, [(i, (i + by) % n) for i in range(n)])


def swap(array, axis):
    return lax.ppermute(array, axis, [(i, i ^ 1) for i in range(lax.axis_size(axis))])


def spread(own, first, second):
    n = own.shape[0]
    h = n // 2
    right, left = shift(own, first, 1), shift(own, first, -1)
    up, down = shift(own, second, 1), shift(own, second, -1)
    right2 = shift(right[:h], first, 1)
    left2 = shift(left[h:], first, -1)
    near = jnp.concatenate([right, left])
    near_up, near_down = shift(near, second, 1), shift(near, second, -1)
    far = jnp.concatenate([right2, left2])
    far_up, far_down = shift(far, second, 1), shift(far, second, -1)
    up2 = shift(jnp.concatenate([up[:h], near_up[:n]]), second, 1)
    down2 = shift(jnp.concatenate([down[h:], near_down[n:]]), second, -1)
    far_up2 = shift(far_up[:h], second, 1)
    far_down2 = shift(far_down[h:], second, -1)
    return [
        (0, 0, 0, n, own, 0),
        (1, 0, 0, n, near, 0),
        (3, 0, 0, n, near, n),
        (2, 0, 0, n, far, 0),
        (0, 1, 0, n, up, 0),
        (0, 3, 0, n, down, 0),
        (1, 1, 0, n, near_up, 0),
        (3, 1, 0, n, near_up, n),
        (1, 3, 0, n, near_down, 0),
        (3, 3, 0, n, near_down, n),
        (2, 1, 0, n, far_up, 0),
        (2, 3, 0, n, far_down, 0),
    ], [
        (0, 2, 0, h, up2, 0),
        (1, 2, 0, n, up2, h),
        (0, 2, h, h, down2, 0),
        (3, 2, 0, n, down2, h),
    ], [
        (2, 2, 0, h, far_up2, 0),
        (2, 2, h, h, far_down2, 0),
    ]


def place(plans, shapes, begun):
    arrays, moves = [], []
    for out, (plan, swapped) in enumerate(plans):
        for back1, back2, row, rows, array, start in plan:
            for k, a in enumerate(arrays):
                if a is array:
                    break
            else:
                k = len(arrays)
                arrays.append(array)
            dy, dx = (back1, back2) if swapped else (back2, back1)
            moves.append((out, dy, dx, row, rows, k, start))
    n_in = len(arrays)

    def body(*refs):
        y, x = lax.axis_index(Y), lax.axis_index(X)
        ins, outs, sem = refs[:n_in], refs[n_in + len(begun) : -1], refs[-1]
        copies = []
        for out, dy, dx, row, rows, k, start in moves:
            lane = lax.rem(y + 4 - dy, 4) * 1024 + lax.rem(x + 4 - dx, 4) * 256
            lane = pl.multiple_of(lane, 256)
            c = pltpu.make_async_copy(
                ins[k].at[pl.ds(start, rows), :],
                outs[out].at[pl.ds(row, rows), pl.ds(lane, 256)],
                sem.at[len(copies)],
            )
            c.start()
            copies.append(c)
        for c in copies:
            c.wait()

    return pl.pallas_call(
        body,
        out_shape=[jax.ShapeDtypeStruct(s, jnp.bfloat16) for s in shapes],
        in_specs=[pl.BlockSpec(memory_space=pl.ANY)] * (n_in + len(begun)),
        out_specs=[pl.BlockSpec(memory_space=pl.ANY)] * len(shapes),
        scratch_shapes=[pltpu.SemaphoreType.DMA((len(moves),))],
        input_output_aliases={n_in + k: k for k in range(len(begun))},
        compiler_params=pltpu.CompilerParams(vmem_limit_bytes=1 << 20),
    )(*(pltpu.with_memory_space_constraint(a, pltpu.VMEM) for a in arrays), *begun)


def shards(
    train_gate, drift_gate, spread_gate, train_up, drift_up, spread_up, norm_train, norm_step
):
    whole_gate = train_gate - learn_rate * (hold_rate * drift_gate + spread_gate)
    whole_up = train_up - learn_rate * (hold_rate * drift_up + spread_up)
    n = whole_gate.shape[1]
    width = lax.axis_size(W)
    squares = (jnp.sum(whole_gate * whole_gate, axis=0), jnp.sum(whole_up * whole_up, axis=0))
    squares, norm_train, norm_step = lax.optimization_barrier((squares, norm_train, norm_step))
    norm = (norm_train + norm_step).astype(jnp.bfloat16).astype(jnp.float32)
    mine = lax.broadcasted_iota(jnp.int32, (width, 1), 0) == lax.axis_index(W)
    norm = jnp.where(mine, norm, 0.0).reshape(-1)
    fill = -2 * n % 128
    told = jnp.concatenate(
        [
            *squares,
            jnp.zeros((fill,), jnp.float32),
            norm,
        ]
    ).reshape(-1, 128)
    heard = lax.all_to_all(
        jnp.broadcast_to(told[None], (16,) + told.shape), FSDP, 0, 0, tiled=True
    )
    last = (2 * n + fill) // 128
    total = jnp.sum(heard[:, :last], axis=0).reshape(-1)
    scale_gate, scale_up = jnp.sqrt(total[:n]), jnp.sqrt(total[n : 2 * n])
    narrow_gate = (whole_gate / scale_gate).astype(jnp.bfloat16).T
    narrow_up = (whole_up / scale_up).astype(jnp.bfloat16).T

    gate_first, gate_next, gate_last = spread(narrow_gate, X, Y)
    up_first, up_next, up_last = spread(narrow_up, Y, X)
    shapes = [(n, 16 * narrow_gate.shape[1])] * 2
    begun = place([(gate_first, False), (up_first, True)], shapes, [])
    begun = place([(gate_next, False), (up_next, True)], shapes, begun)
    serving_gate, serving_up = place([(gate_last, False), (up_last, True)], shapes, begun)

    norms = heard[:, last:].astype(jnp.bfloat16).reshape(-1, 128)
    by, step = 1, 0
    while by < width:
        step += 1
        more = shift(norms, W, by) if by > 1 else swap(norms, W)
        norms = norms + more
        by *= 2
    norms = norms.reshape(-1)
    return (serving_gate.T, serving_up.T, scale_gate, scale_up, norms, whole_gate, whole_up)


def solution(mesh):
    split = Mesh(mesh.devices.reshape(4, 4, mesh.shape["width"]), (Y, X, W))
    weight, gain = P(FSDP, W), P(FSDP_WIDTH)
    return jax.shard_map(
        shards,
        mesh=split,
        in_specs=(weight,) * 6 + (gain,) * 2,
        out_specs=(P(None, W), P(None, W), P(W), P(W), P(), weight, weight),
        check_vma=False,
    )
```
